256 devices in a mesh: grp: 2 (over z), row: 64 (over y, x), col: 2 (over core).
Axes of the slice: x: 8, y: 8, z: 2, core: 2. Of those that a mesh axis runs over, the one named last changes fastest.
The devices are a block of a 8x8x16 slice.
Arguments:
- factors: bfloat16 [2, 12288, 6144], P(None, ('grp', 'row'), 'col'), parts along dimension 1, may hold values from -6 to 6
- orbitals: bfloat16 [12288, 1024], P(('grp', 'row'), 'col'), parts along dimension 0, may hold values from -0.02734375 to 0.02734375
- field_term: bfloat16 [12288, 6144], P(('grp', 'row'), 'col'), parts along dimension 0, may hold values from -1.5 to 1.5
Outputs:
- fock_matrix: bfloat16 [12288, 6144], P(('grp', 'row'), 'col'), parts along dimension 0
The draws below stay inside these ranges and needn't reach their ends.
There are 2 independent parts, one for each index of `grp`. The reference program is written for one: setup_inputs(seed, part) draws one part's arguments, and reference() takes and returns one part's arrays. A program takes and returns all parts, laid end to end along the dimension named above; each array names one. Nothing has to cross between parts.
All inputs are finite; a program needn't handle non-finite values.
Results may differ from the reference program's by a relative error of at most 0.02.
Values may be sent and summed in bfloat16 or wider, within the bound.
A program may use at most 64 MiB of HBM per device.

```python
import jax
import jax.numpy as jnp

N = 6144
NOCC = 1024
NAUX = 2


def steps_of(rng, extent, pieces, smallest, top_value):
    gain, own = 1.0, jax.random.fold_in(rng, 6)
    for axis_at, shards_of in pieces:
        draws = jnp.exp(jax.random.uniform(jax.random.fold_in(own, axis_at), (shards_of,), jnp.float32, smallest / len(pieces), top_value / len(pieces)))
        gain = gain * jnp.repeat(draws, extent[axis_at] // shards_of).reshape([-1 if axis == axis_at else 1 for axis in range(len(extent))])
    return gain


def normal_values(stream_key, shape, width, limit, shards=(), kind=jnp.bfloat16):
    loudness = steps_of(stream_key, shape, shards, -0.22, 0.18) if shards else 1.0
    array = jax.random.normal(stream_key, shape, jnp.float32) * width * loudness
    return jnp.minimum(jnp.maximum(array, -limit), limit).astype(kind)


def setup_inputs(seed: int = 0, part: int = 0) -> dict:
    streams_of = jax.random.split(jax.random.key(seed), 4)
    part_splits = jax.random.split(jax.random.fold_in(streams_of[3], part), 4)
    return {
        "factors": normal_values(part_splits[0], (NAUX, N, N), 1.0, 6.0, ((1, 64), (2, 2))),
        "orbitals": normal_values(part_splits[1], (N, NOCC), (N * 8) ** -0.5, 0.02734375, ((0, 64), (1, 2))),
        "field_term": normal_values(part_splits[2], (N, N), 0.25, 1.5, ((0, 64), (1, 2))),
    }


def reference(factors, orbitals, field_term):
    orbit_wide = orbitals.astype(jnp.float32)
    exchange = jnp.zeros((N, N), jnp.float32)
    coulomb = jnp.zeros((N, N), jnp.float32)
    for aux in range(NAUX):
        half_aux = jnp.dot(factors[aux], orbitals, preferred_element_type=jnp.float32).astype(jnp.bfloat16)
        gamma_aux = jnp.sum(half_aux.astype(jnp.float32) * orbit_wide)
        exchange = exchange + jnp.dot(half_aux, half_aux.T, preferred_element_type=jnp.float32)
        coulomb = coulomb + gamma_aux * factors[aux].astype(jnp.float32)
    fock_matrix = field_term.astype(jnp.float32) + coulomb - 0.25 * exchange
    return fock_matrix.astype(jnp.bfloat16)
```

```python
import functools
import math

import jax
import jax.numpy as jnp
from jax import lax
from jax.experimental import pallas as pl
from jax.experimental.pallas import tpu as pltpu
from jax.sharding import Mesh
from jax.sharding import PartitionSpec as P

GRP_ROW = ("grp", "row_0", "row_1")
AXES = ("row_1", "row_0")
LANES = 128


def offset_of(unit):
    return ((unit + 1) // 2) * (2 * (unit % 2) - 1)


def fock_kernel(
    side, f_hbm, c_hbm, t_hbm, o_hbm,
    bfull, blocal, call, hacc, rbuf, cbuf, ksx, ksy, krecv, field, base, out, gx, gy, gd,
    loc, osem, bsem, s1s, s1r, s2s, s2r, hs, hr, ds_, dr, xs, ys, kr, gxs, gxr, gys, gyr, gds, gdr,
):
    naux, n, ncol = f_hbm.shape
    ni = c_hbm.shape[1]
    w = ni // 2
    far = side // 2
    y, x, c = (lax.axis_index(a) for a in ("row_0", "row_1", "col"))
    pos = (x, y)
    sib = {"col": 1 - c}

    def at(p, off):
        return lax.rem(p + (off + side), side)

    def neighbour(axis, off):
        return {AXES[axis]: at(pos[axis], off)}

    def remote(src, dst, ssem, rsem, device):
        return pltpu.make_async_remote_copy(
            src_ref=src, dst_ref=dst, send_sem=ssem, recv_sem=rsem,
            device_id=device, device_id_type=pl.DeviceIdType.MESH,
        )

    def rows(k, d):
        if k < far:
            return pl.ds(0, n)
        return pl.ds(0, n // 2) if d > 0 else pl.ds(n // 2, n // 2)

    my_slot = y * side + x
    own_c = [
        pltpu.make_async_copy(c_hbm.at[:, pl.ds(h * w, w)], call.at[h, my_slot], loc.at[h])
        for h in range(2)
    ]
    half_cols = pl.ds(pl.multiple_of(c * ncol, LANES), ncol)
    own_b = pltpu.make_async_copy(f_hbm, bfull.at[:, :, half_cols], loc.at[2])
    own_b2 = pltpu.make_async_copy(f_hbm, blocal, loc.at[3])
    own_t = pltpu.make_async_copy(t_hbm, field, loc.at[4])
    for copy in (*own_c, own_b, own_b2, own_t):
        copy.start()
    barrier = pltpu.get_barrier_semaphore()

    def hello(device):
        pl.semaphore_signal(
            barrier, inc=1, device_id=device, device_id_type=pl.DeviceIdType.MESH
        )

    hello(sib)
    for off in range(1, side):
        hello(neighbour(0, off))
        hello(neighbour(1, off))
        hello({**neighbour(1, off), **sib})
    pl.semaphore_wait(barrier, 3 * (side - 1) + 1)

    def slot(h, off1, off2):
        if h == 0:
            return at(y, off2) * side + at(x, off1)
        return at(y, off1) * side + at(x, off2)

    def s1(h, k, d, off):
        ref = call.at[h, slot(h, off, 0), rows(k, d)]
        i = (h, (1 - d) // 2, k - 1)
        return remote(ref, ref, s1s.at[i], s1r.at[i], neighbour(h, d))

    def s2(h, k, d, unit, off):
        ref = call.at[h, slot(h, offset_of(unit), off), rows(k, d)]
        di = (1 - d) // 2
        return remote(
            ref, ref, s2s.at[h, di, k - 1, unit], s2r.at[h, di, k - 1, unit], neighbour(1 - h, d)
        )

    both = [(h, d) for h in range(2) for d in (1, -1)]
    for copy in own_c:
        copy.wait()
    for h, d in both:
        s1(h, 1, d, 0).start()
    for h, d in both:
        s2(h, 1, d, 0, 0).start()
    own_b.wait()
    mine = bfull.at[:, :, half_cols]
    swap_b = remote(mine, mine, bsem.at[0], bsem.at[1], sib)
    swap_b.start()
    for k in range(1, far + 1):
        for h, d in both:
            s1(h, k, d, -k * d).wait_recv()
            if k < far:
                s1(h, k + 1, d, -k * d).start()
                unit = 2 * k if d > 0 else 2 * k - 1
                for e in (1, -1):
                    s2(h, 1, e, unit, 0).start()
            elif d < 0:
                for e in (1, -1):
                    s2(h, 1, e, 2 * k - 1, 0).start()
    for k in range(1, far + 1):

        def hop(unit, carry, k=k):
            for h, d in both:
                s2(h, k, d, unit, -k * d).wait_recv()
                if k < far:
                    s2(h, k + 1, d, unit, -k * d).start()
            return carry

        lax.fori_loop(0, side, hop, 0)

    theirs = bfull.at[:, :, pl.ds(pl.multiple_of((1 - c) * ncol, LANES), ncol)]
    remote(theirs, theirs, bsem.at[0], bsem.at[1], sib).wait_recv()
    hacc[...] = jnp.zeros_like(hacc)
    deep = side * n

    @pl.loop(0, side)
    def _(i):
        left = bfull[:, :, pl.ds(pl.multiple_of(i * deep, LANES), deep)].reshape(naux * n, deep)
        for h in range(2):
            right = call[h, pl.ds(i * side, side)].reshape(deep, w)
            hacc[h] += jnp.dot(left, right, preferred_element_type=jnp.float32)

    sums = [jnp.zeros((1, 1), jnp.float32) for _ in range(naux)]
    for h in range(2):
        own = call[h, my_slot].astype(jnp.float32)
        for p in range(naux):
            block = hacc[h, pl.ds(p * n, n), :].astype(jnp.bfloat16)
            lanes = pl.ds(p * ni + h * w, w)
            rbuf[c, x, pl.ds(0, n), lanes] = block
            cbuf[c, y, pl.ds(0, n), lanes] = block
            sums[p] += jnp.sum(block.astype(jnp.float32) * own, keepdims=True)

    bufs = (rbuf, cbuf)
    units = 2 * naux

    def lanes_of(u):
        h, p = divmod(u, naux)
        return pl.ds(p * ni + h * w, w)

    def ring(a, k, d, u, off):
        ref = bufs[a].at[c, at(pos[a], off), rows(k, d), lanes_of(u)]
        i = (a, (1 - d) // 2, k - 1, u)
        return remote(ref, ref, hs.at[i], hr.at[i], neighbour(a, d))

    def share(a, off, u, core):
        ref = bufs[a].at[core, at(pos[a], off), pl.ds(0, n), lanes_of(u)]
        i = (a, off % side, u)
        return remote(ref, ref, ds_.at[i], dr.at[i], sib)

    for u in range(units):
        for a, d in both:
            ring(a, 1, d, u, 0).start()
    for u in range(units):
        for a in range(2):
            share(a, 0, u, c).start()

    line = lax.broadcasted_iota(jnp.int32, (8, LANES), 0)
    tile = jnp.zeros((8, LANES), jnp.float32)
    for p in range(naux):
        tile = jnp.where(line == p, sums[p], tile)
    gx[x] = tile

    def gamma_copy(a, off):
        buf, ss, rs = ((gx, gxs, gxr), (gy, gys, gyr))[a]
        return remote(buf.at[pos[a]], buf.at[pos[a]], ss.at[off - 1], rs.at[off - 1], neighbour(a, off))

    def gamma_wait(a, off):
        buf, ss, rs = ((gx, gxs, gxr), (gy, gys, gyr))[a]
        ref = buf.at[at(pos[a], -off)]
        remote(ref, ref, ss.at[off - 1], rs.at[off - 1], neighbour(a, off)).wait_recv()

    for off in range(1, side):
        gamma_copy(0, off).start()

    for k in range(1, far + 1):
        for u in range(units):
            for a, d in both:
                ring(a, k, d, u, -k * d).wait_recv()
                if k < far:
                    ring(a, k + 1, d, u, -k * d).start()
                    share(a, -k * d, u, c).start()
                elif d < 0:
                    share(a, far, u, c).start()
        if k == 2:
            for off in range(1, side):
                gamma_wait(0, off)
            gy[y] = jnp.sum(gx[...], axis=0)
            for off in range(1, side):
                gamma_copy(1, off).start()
    for off in range(1, side):
        gamma_wait(1, off)
    gd[c] = jnp.sum(gy[...], axis=0)
    swap_g = remote(gd.at[c], gd.at[c], gds, gdr, sib)
    swap_g.start()
    for a in range(2):
        for off in range(side):
            for u in range(units):
                share(a, off, u, 1 - c).wait_recv()

    deep = naux * ni
    first = c * far
    nt = (((1,), (1,)), ((), ()))

    def by_x(target_x, block_y):
        return along_x(at(x, -target_x), at(block_y, -y))

    def along_x(dx, dy):
        a, b = jnp.minimum(dx, side - dx), jnp.minimum(dy, side - dy)
        return (a < b) | ((a == b) & ((dx < far) == (dy < far)))

    def send_x(q, i):
        return remote(
            ksx.at[q, i], krecv.at[q, x], xs.at[q, i], kr.at[q, x], {"row_1": i}
        )

    def x_sent(q, i):
        return (i != x) & (first + q != y) & by_x(i, first + q)

    y_half = y // far

    def send_y(q, i):
        there = lax.rem(y, far)
        return remote(
            ksy.at[q, i], krecv.at[there, i], ys.at[q, i], kr.at[there, i],
            {"row_0": first + q, "col": y_half},
        )

    def y_sent(q, i):
        return (i != x) & (first + q != y) & jnp.logical_not(
            along_x(at(i, -x), at(y, -(first + q)))
        )

    for j in range(far // 2):
        acc = None
        for core in range(2):
            left = rbuf[core, :, pl.ds(0, n), :].reshape(side * n, deep)
            right = cbuf[core, pl.ds(first + 2 * j, 2)].reshape(2 * LANES, deep)
            term = lax.dot_general(left, right, nt, preferred_element_type=jnp.float32)
            acc = term if acc is None else acc + term
        for i in range(2):
            ksx[2 * j + i] = (
                acc[:, i * LANES : (i + 1) * LANES].astype(jnp.bfloat16).reshape(side, n, LANES)
            )
        for i in range(2):

            @pl.loop(0, side)
            def _(t, q=2 * j + i):
                pl.when(x_sent(q, t))(lambda: send_x(q, t).start())

    for j in range(side // 2):
        acc = None
        for core in range(2):
            left = cbuf[core, pl.ds(first, far), pl.ds(0, n), :].reshape(far * n, deep)
            right = rbuf[core, pl.ds(2 * j, 2)].reshape(2 * LANES, deep)
            term = lax.dot_general(left, right, nt, preferred_element_type=jnp.float32)
            acc = term if acc is None else acc + term
        for i in range(2):
            part = acc[:, i * LANES : (i + 1) * LANES].astype(jnp.bfloat16).reshape(far, n, LANES)
            ksy[:, 2 * j + i] = part
        for i in range(2):

            @pl.loop(0, far)
            def _(q, t=2 * j + i):
                pl.when(y_sent(q, t))(lambda: send_y(q, t).start())

    for q in range(far):
        krecv[q, x] = ksx[q, x]

        @pl.when(first + q == y)
        def _(q=q):
            @pl.loop(0, side)
            def _(i):
                @pl.when(i != x)
                def _():
                    krecv[q, i] = ksy[q, i]

    own_b2.wait()
    own_t.wait()
    other = gd.at[1 - c]
    remote(other, other, gds, gdr, sib).wait_recv()
    gamma = jnp.sum(gd[...], axis=0)
    width = side * n

    @pl.loop(0, far)
    def _(q):
        cols = pl.ds(pl.multiple_of(q * width, LANES), width)
        total = field[:, cols].astype(jnp.float32)
        for p in range(naux):
            total += gamma[p : p + 1, 0:1] * blocal[p, :, cols].astype(jnp.float32)
        base[:, cols] = total

    lane = lax.broadcasted_iota(jnp.int32, (n, LANES), 1)
    for q in range(far):

        @pl.loop(0, side)
        def _(i, q=q):
            @pl.when((i != x) & (first + q != y))
            def _():
                ref = krecv.at[q, i]
                remote(ref, ref, xs.at[q, i], kr.at[q, i], sib).wait_recv()

        for g in range(side // 4):
            b = [krecv[q, 4 * g + i].astype(jnp.float32) for i in range(4)]
            r = [b[0]] + [pltpu.roll(b[i], LANES - 32 * i, 1) for i in range(1, 4)]
            for t in range(3):
                start = q * width + g * 4 * n + t * LANES
                cols = pl.ds(start, LANES)
                piece = jnp.where(lane < n - 32 * t, r[t], r[t + 1])
                out[:, cols] = (base[:, cols] - 0.25 * piece).astype(out.dtype)
        cols = pl.ds(q * width, width)
        pltpu.make_async_copy(out.at[:, cols], o_hbm.at[:, cols], osem.at[q]).start()

    for k in range(1, far + 1):
        for h, d in both:
            s1(h, k, d, -(k - 1) * d).wait_send()

        def sent(unit, carry, k=k):
            for h, d in both:
                s2(h, k, d, unit, -(k - 1) * d).wait_send()
            return carry

        lax.fori_loop(0, side, sent, 0)
        for u in range(units):
            for a, d in both:
                ring(a, k, d, u, -(k - 1) * d).wait_send()
    swap_b.wait_send()
    swap_g.wait_send()
    for off in range(1, side):
        gamma_copy(0, off).wait_send()
        gamma_copy(1, off).wait_send()
    for a in range(2):
        for off in range(side):
            for u in range(units):
                share(a, off, u, c).wait_send()
    for q in range(far):

        @pl.loop(0, side)
        def _(i, q=q):
            pl.when(x_sent(q, i))(lambda: send_x(q, i).wait_send())
            pl.when(y_sent(q, i))(lambda: send_y(q, i).wait_send())

    for q in range(far):
        cols = pl.ds(q * width, width)
        pltpu.make_async_copy(out.at[:, cols], o_hbm.at[:, cols], osem.at[q]).wait()


def shards(side, factors, orbitals, field_term):
    naux, n, ncol = factors.shape
    ni = orbitals.shape[1]
    w = ni // 2
    far = side // 2
    units = 2 * naux
    bf16, f32, dma = jnp.bfloat16, jnp.float32, pltpu.SemaphoreType.DMA
    hbm = pl.BlockSpec(memory_space=pl.ANY)
    return pl.pallas_call(
        functools.partial(fock_kernel, side),
        out_shape=jax.ShapeDtypeStruct((n, ncol), bf16),
        in_specs=[hbm] * 3,
        out_specs=hbm,
        scratch_shapes=[
            pltpu.VMEM((naux, n, 2 * ncol), bf16),
            pltpu.VMEM((naux, n, ncol), bf16),
            pltpu.VMEM((2, side * side, n, w), bf16),
            pltpu.VMEM((2, naux * n, w), f32),
            pltpu.VMEM((2, side, LANES, naux * ni), bf16),
            pltpu.VMEM((2, side, LANES, naux * ni), bf16),
            pltpu.VMEM((far, side, n, LANES), bf16),
            pltpu.VMEM((far, side, n, LANES), bf16),
            pltpu.VMEM((far, side, n, LANES), bf16),
            pltpu.VMEM((n, ncol), bf16),
            pltpu.VMEM((n, ncol), f32),
            pltpu.VMEM((n, ncol), bf16),
            pltpu.VMEM((side, 8, LANES), f32),
            pltpu.VMEM((side, 8, LANES), f32),
            pltpu.VMEM((2, 8, LANES), f32),
            dma((5,)),
            dma((far,)),
            dma((2,)),
            dma((2, 2, far)),
            dma((2, 2, far)),
            dma((2, 2, far, side)),
            dma((2, 2, far, side)),
            dma((2, 2, far, units)),
            dma((2, 2, far, units)),
            dma((2, side, units)),
            dma((2, side, units)),
            dma((far, side)),
            dma((far, side)),
            dma((far, side)),
            dma((side - 1,)),
            dma((side - 1,)),
            dma((side - 1,)),
            dma((side - 1,)),
            dma,
            dma,
        ],
        compiler_params=pltpu.CompilerParams(
            collective_id=0, has_side_effects=True, vmem_limit_bytes=60 * 1024 * 1024
        ),
        name="fock",
    )(factors, orbitals, field_term)


def solution(mesh):
    side = math.isqrt(mesh.shape["row"])
    finer = Mesh(
        mesh.devices.reshape(mesh.shape["grp"], side, side, mesh.shape["col"]),
        ("grp", "row_0", "row_1", "col"),
    )
    return jax.shard_map(
        functools.partial(shards, side),
        mesh=finer,
        in_specs=(P(None, GRP_ROW, "col"), P(GRP_ROW, "col"), P(GRP_ROW, "col")),
        out_specs=P(GRP_ROW, "col"),
        check_vma=False,
    )
```

```python
import functools
import math

import jax
import jax.numpy as jnp
from jax import lax
from jax.experimental import pallas as pl
from jax.experimental.pallas import tpu as pltpu
from jax.sharding import Mesh
from jax.sharding import PartitionSpec as P

GRP_ROW = ("grp", "row_0", "row_1")
AXES = ("row_1", "row_0")
LANES = 128
CHUNKS = 2


def offset_of(unit):
    return ((unit + 1) // 2) * (2 * (unit % 2) - 1)


def fock_kernel(
    side, chunks, f_hbm, c_hbm, t_hbm, o_hbm,
    bfull, blocal, call, hacc, rbuf, cbuf, kxacc, kyacc, ksx, ksy, krx, kry, field, base, out, gx, gy, gd,
    loc, osem, bsem, s1s, s1r, s2s, s2r, hs, hr, ds_, dr, xs, ys, krxs, krys, gxs, gxr, gys, gyr, gds, gdr,
):
    naux, n, ncol = f_hbm.shape
    ni = c_hbm.shape[1]
    wide = ni // chunks
    w = wide // 2
    far = side // 2
    near = far // 2
    y, x, c = (lax.axis_index(a) for a in ("row_0", "row_1", "col"))
    pos = (x, y)
    sib = {"col": 1 - c}

    def at(p, off):
        return lax.rem(p + (off + side), side)

    def neighbour(axis, off):
        return {AXES[axis]: at(pos[axis], off)}

    def remote(src, dst, ssem, rsem, device):
        return pltpu.make_async_remote_copy(
            src_ref=src, dst_ref=dst, send_sem=ssem, recv_sem=rsem,
            device_id=device, device_id_type=pl.DeviceIdType.MESH,
        )

    def rows(k, d):
        if k < far:
            return pl.ds(0, n)
        return pl.ds(0, n // 2) if d > 0 else pl.ds(n // 2, n // 2)

    my_slot = y * side + x
    own_c = [
        pltpu.make_async_copy(c_hbm.at[:, pl.ds(q * wide, wide)], call.at[q, my_slot], loc.at[q])
        for q in range(chunks)
    ]
    half_cols = pl.ds(pl.multiple_of(c * ncol, LANES), ncol)
    own_b = pltpu.make_async_copy(f_hbm, bfull.at[:, :, half_cols], loc.at[chunks])
    own_b2 = pltpu.make_async_copy(f_hbm, blocal, loc.at[chunks + 1])
    own_t = pltpu.make_async_copy(t_hbm, field, loc.at[chunks + 2])
    for copy in (*own_c, own_b, own_b2, own_t):
        copy.start()
    barrier = pltpu.get_barrier_semaphore()
    friends = [sib] + [neighbour(axis, off) for axis in range(2) for off in (1, -1)]
    for device in friends:
        pl.semaphore_signal(
            barrier, inc=1, device_id=device, device_id_type=pl.DeviceIdType.MESH
        )
    pl.semaphore_wait(barrier, len(friends))

    both = [(h, d) for h in range(2) for d in (1, -1)]

    def slot(h, off1, off2):
        if h == 0:
            return at(y, off2) * side + at(x, off1)
        return at(y, off1) * side + at(x, off2)

    def s1(q, h, k, d, off):
        ref = call.at[q, slot(h, off, 0), rows(k, d), pl.ds(h * w, w)]
        i = (q, h, (1 - d) // 2, k - 1)
        return remote(ref, ref, s1s.at[i], s1r.at[i], neighbour(h, d))

    def s2(q, h, k, d, unit, off):
        ref = call.at[q, slot(h, offset_of(unit), off), rows(k, d), pl.ds(h * w, w)]
        i = (q, h, (1 - d) // 2, k - 1, unit)
        return remote(ref, ref, s2s.at[i], s2r.at[i], neighbour(1 - h, d))

    def begin(q):
        own_c[q].wait()
        for h, d in both:
            s1(q, h, 1, d, 0).start()
        for h, d in both:
            s2(q, h, 1, d, 0, 0).start()

    def first_hop(q, k):
        for h, d in both:
            s1(q, h, k, d, -k * d).wait_recv()
            if k < far:
                s1(q, h, k + 1, d, -k * d).start()
                unit = 2 * k if d > 0 else 2 * k - 1
                for e in (1, -1):
                    s2(q, h, 1, e, unit, 0).start()
            elif d < 0:
                for e in (1, -1):
                    s2(q, h, 1, e, 2 * k - 1, 0).start()

    def second_hop(q, k):
        def hop(unit, carry):
            for h, d in both:
                s2(q, h, k, d, unit, -k * d).wait_recv()
                if k < far:
                    s2(q, h, k + 1, d, unit, -k * d).start()
            return carry

        lax.fori_loop(0, side, hop, 0)

    deep = side * n
    sums = [jnp.zeros((1, 1), jnp.float32) for _ in range(naux)]

    def lanes_of(q, p):
        return pl.ds((q * naux + p) * wide, wide)

    def half_transform(q):
        hacc[...] = jnp.zeros_like(hacc)

        @pl.loop(0, side)
        def _(i):
            left = bfull[:, :, pl.ds(pl.multiple_of(i * deep, LANES), deep)]
            right = call[q, pl.ds(i * side, side)].reshape(deep, wide)
            hacc[...] += jnp.dot(
                left.reshape(naux * n, deep), right, preferred_element_type=jnp.float32
            )

        own = call[q, my_slot].astype(jnp.float32)
        for p in range(naux):
            block = hacc[pl.ds(p * n, n), :].astype(jnp.bfloat16)
            rbuf[c, x, :, lanes_of(q, p)] = block
            cbuf[c, near, pl.ds(0, n), lanes_of(q, p)] = block
            sums[p] += jnp.sum(block.astype(jnp.float32) * own, keepdims=True)

    units = 2 * naux

    def part(a, core, off, rs, q, u):
        lanes = pl.ds((q * units + u) * w, w)
        if a == 0:
            return rbuf.at[core, at(x, off), rs, lanes]
        return cbuf.at[core, (off + near) % side, rs, lanes]

    def ring(q, a, k, d, u):
        i = (q, a, (1 - d) // 2, k - 1, u)
        src = part(a, c, -(k - 1) * d, rows(k, d), q, u)
        dst = src if a == 0 else part(a, c, -k * d, rows(k, d), q, u)
        return remote(src, dst, hs.at[i], hr.at[i], neighbour(a, d))

    def ring_in(q, a, k, d, u):
        i = (q, a, (1 - d) // 2, k - 1, u)
        ref = part(a, c, -k * d, rows(k, d), q, u)
        return remote(ref, ref, hs.at[i], hr.at[i], neighbour(a, d))

    def share(q, a, off, u, core):
        ref = part(a, core, off, pl.ds(0, n), q, u)
        i = (q, a, off % side, u)
        return remote(ref, ref, ds_.at[i], dr.at[i], sib)

    def begin_ring(q):
        for u in range(units):
            for a, d in both:
                ring(q, a, 1, d, u).start()
        for u in range(units):
            for a in range(2):
                share(q, a, 0, u, c).start()

    def ring_hop(q, k):
        for u in range(units):
            for a, d in both:
                ring_in(q, a, k, d, u).wait_recv()
                if k < far:
                    ring(q, a, k + 1, d, u).start()
                    share(q, a, -k * d, u, c).start()
                elif d < 0:
                    share(q, a, far, u, c).start()

    def shared(q):
        for a in range(2):
            for off in range(side):
                for u in range(units):
                    share(q, a, off, u, 1 - c).wait_recv()

    first = c * far
    nt = (((1,), (1,)), ((), ()))
    band = 2 * near + 1
    rest = side - band

    def products(q):
        lanes = pl.ds(q * naux * wide, naux * wide)
        span = naux * wide
        kx = ky = None
        for core in range(2):
            ours = rbuf[core, pl.ds(first, far), :, lanes].reshape(far * n, span)
            close = cbuf[core, pl.ds(0, band), pl.ds(0, n), lanes].reshape(band * n, span)
            away = cbuf[core, pl.ds(band, rest), :, lanes].reshape(rest * LANES, span)
            tx = lax.dot_general(ours, away, nt, preferred_element_type=jnp.float32)
            ty = lax.dot_general(close, ours, nt, preferred_element_type=jnp.float32)
            kx = tx if kx is None else kx + tx
            ky = ty if ky is None else ky + ty
        return kx, ky

    gammas = ((gx, gxs, gxr), (gy, gys, gyr))

    def gamma_copy(a, off):
        buf, ss, rs = gammas[a]
        ref = buf.at[pos[a]]
        return remote(ref, ref, ss.at[off - 1], rs.at[off - 1], neighbour(a, off))

    def gamma_wait(a, off):
        buf, ss, rs = gammas[a]
        ref = buf.at[at(pos[a], -off)]
        remote(ref, ref, ss.at[off - 1], rs.at[off - 1], neighbour(a, off)).wait_recv()

    swap_g = remote(gd.at[c], gd.at[c], gds, gdr, sib)

    mine = bfull.at[:, :, half_cols]
    theirs = bfull.at[:, :, pl.ds(pl.multiple_of((1 - c) * ncol, LANES), ncol)]
    swap_b = remote(mine, mine, bsem.at[0], bsem.at[1], sib)

    begin(0)
    own_b.wait()
    swap_b.start()
    for k in range(1, far + 1):
        first_hop(0, k)
    remote(theirs, theirs, bsem.at[0], bsem.at[1], sib).wait_recv()
    last = chunks - 1
    for q in range(chunks):
        if q < last:
            begin(q + 1)
        for k in range(1, far + 1):
            second_hop(q, k)
            if q > 0:
                ring_hop(q - 1, k)
            if q < last:
                first_hop(q + 1, k)
        half_transform(q)
        begin_ring(q)
        if q > 0:
            shared(q - 1)
            kx, ky = products(q - 1)
            if q > 1:
                kx, ky = kxacc[...] + kx, kyacc[...] + ky
            kxacc[...] = kx
            kyacc[...] = ky

    line = lax.broadcasted_iota(jnp.int32, (8, LANES), 0)
    tile = jnp.zeros((8, LANES), jnp.float32)
    for p in range(naux):
        tile = jnp.where(line == p, sums[p], tile)
    gx[x] = tile
    for off in range(1, side):
        gamma_copy(0, off).start()
    for k in range(1, far + 1):
        ring_hop(last, k)
        if k == 2:
            for off in range(1, side):
                gamma_wait(0, off)
            gy[y] = jnp.sum(gx[...], axis=0)
            for off in range(1, side):
                gamma_copy(1, off).start()
    for off in range(1, side):
        gamma_wait(1, off)
    gd[c] = jnp.sum(gy[...], axis=0)
    swap_g.start()
    shared(last)
    kx, ky = products(last)
    if last > 0:
        kx, ky = kxacc[...] + kx, kyacc[...] + ky

    y_half = y // far
    y_low = lax.rem(y, far)

    def x_block(j):
        other = at(y, near + 1 + j)
        return other // far, lax.rem(other, far)

    def send_x(j, i):
        core, low = x_block(j)
        return remote(
            ksx.at[j, i], krx.at[low, x], xs.at[j, i], krxs.at[low, x],
            {"row_1": first + i, "col": core},
        )

    def x_stays(j, i):
        core, _ = x_block(j)
        return (first + i == x) & (core == c)

    def send_y(m):
        return remote(
            ksy.at[m], kry.at[y_low, c], ys.at[m], krys.at[y_low, c],
            {"row_0": at(y, m - near), "col": y_half},
        )

    y_stays = y_half == c
    for j in range(rest):
        piece = kx[:, j * LANES : (j + 1) * LANES].astype(jnp.bfloat16)
        ksx[j] = piece.reshape(far, n, LANES)
        for i in range(far):
            pl.when(jnp.logical_not(x_stays(j, i)))(lambda j=j, i=i: send_x(j, i).start())
    ksy[...] = ky.astype(jnp.bfloat16).reshape(band, n, far * n)
    for m in range(band):
        if m == near:
            pl.when(jnp.logical_not(y_stays))(lambda m=m: send_y(m).start())
        else:
            send_y(m).start()

    for j in range(rest):
        for i in range(far):

            @pl.when(x_stays(j, i))
            def _(j=j, i=i):
                krx[x_block(j)[1], x] = ksx[j, i]

    @pl.when(y_stays)
    def _():
        kry[y_low, c] = ksy[near]

    own_b2.wait()
    own_t.wait()
    other = gd.at[1 - c]
    remote(other, other, gds, gdr, sib).wait_recv()
    gamma = jnp.sum(gd[...], axis=0)
    width = side * n

    @pl.loop(0, far)
    def _(q):
        cols = pl.ds(pl.multiple_of(q * width, LANES), width)
        total = field[:, cols].astype(jnp.float32)
        for p in range(naux):
            total += gamma[p : p + 1, 0:1] * blocal[p, :, cols].astype(jnp.float32)
        base[:, cols] = total

    lane = lax.broadcasted_iota(jnp.int32, (n, LANES), 1)
    for q in range(far):
        dy = at(first + q, -y)
        by_x = (dy > near) & (dy < side - near)

        @pl.when(by_x)
        def _(q=q):
            @pl.loop(0, side)
            def _(i):
                @pl.when((i != x) | (x // far != c))
                def _():
                    ref = krx.at[q, i]
                    remote(ref, ref, xs.at[0, 0], krxs.at[q, i], sib).wait_recv()

            for g in range(side // 4):
                b = [krx[q, 4 * g + i].astype(jnp.float32) for i in range(4)]
                r = [b[0]] + [pltpu.roll(b[i], LANES - 32 * i, 1) for i in range(1, 4)]
                for t in range(3):
                    cols = pl.ds(q * width + g * 4 * n + t * LANES, LANES)
                    piece = jnp.where(lane < n - 32 * t, r[t], r[t + 1])
                    out[:, cols] = (base[:, cols] - 0.25 * piece).astype(out.dtype)

        @pl.when(jnp.logical_not(by_x))
        def _(q=q, dy=dy):
            for g in range(2):

                @pl.when((dy != 0) | (c != g))
                def _(g=g):
                    ref = kry.at[q, g]
                    remote(ref, ref, ys.at[0], krys.at[q, g], sib).wait_recv()

                cols = pl.ds(q * width + g * far * n, far * n)
                piece = kry[q, g].astype(jnp.float32)
                out[:, cols] = (base[:, cols] - 0.25 * piece).astype(out.dtype)

        cols = pl.ds(q * width, width)
        pltpu.make_async_copy(out.at[:, cols], o_hbm.at[:, cols], osem.at[q]).start()

    for q in range(chunks):
        for k in range(1, far + 1):
            for h, d in both:
                s1(q, h, k, d, -(k - 1) * d).wait_send()

            def sent(unit, carry, q=q, k=k):
                for h, d in both:
                    s2(q, h, k, d, unit, -(k - 1) * d).wait_send()
                return carry

            lax.fori_loop(0, side, sent, 0)
            for u in range(units):
                for a, d in both:
                    ring(q, a, k, d, u).wait_send()
        for a in range(2):
            for off in range(side):
                for u in range(units):
                    share(q, a, off, u, c).wait_send()
    swap_b.wait_send()
    swap_g.wait_send()
    for off in range(1, side):
        gamma_copy(0, off).wait_send()
        gamma_copy(1, off).wait_send()
    for j in range(rest):
        for i in range(far):
            pl.when(jnp.logical_not(x_stays(j, i)))(lambda j=j, i=i: send_x(j, i).wait_send())
    for m in range(band):
        if m == near:
            pl.when(jnp.logical_not(y_stays))(lambda m=m: send_y(m).wait_send())
        else:
            send_y(m).wait_send()
    for q in range(far):
        cols = pl.ds(q * width, width)
        pltpu.make_async_copy(out.at[:, cols], o_hbm.at[:, cols], osem.at[q]).wait()


def shards(side, chunks, factors, orbitals, field_term):
    naux, n, ncol = factors.shape
    ni = orbitals.shape[1]
    wide = ni // chunks
    far = side // 2
    band = 2 * (far // 2) + 1
    rest = side - band
    units = 2 * naux
    bf16, f32, dma = jnp.bfloat16, jnp.float32, pltpu.SemaphoreType.DMA
    hbm = pl.BlockSpec(memory_space=pl.ANY)
    return pl.pallas_call(
        functools.partial(fock_kernel, side, chunks),
        out_shape=jax.ShapeDtypeStruct((n, ncol), bf16),
        in_specs=[hbm] * 3,
        out_specs=hbm,
        scratch_shapes=[
            pltpu.VMEM((naux, n, 2 * ncol), bf16),
            pltpu.VMEM((naux, n, ncol), bf16),
            pltpu.VMEM((chunks, side * side, n, wide), bf16),
            pltpu.VMEM((naux * n, wide), f32),
            pltpu.VMEM((2, side, n, naux * ni), bf16),
            pltpu.VMEM((2, side, LANES, naux * ni), bf16),
            pltpu.VMEM((far * n, rest * LANES), f32),
            pltpu.VMEM((band * n, far * n), f32),
            pltpu.VMEM((rest, far, n, LANES), bf16),
            pltpu.VMEM((band, n, far * n), bf16),
            pltpu.VMEM((far, side, n, LANES), bf16),
            pltpu.VMEM((far, 2, n, far * n), bf16),
            pltpu.VMEM((n, ncol), bf16),
            pltpu.VMEM((n, ncol), f32),
            pltpu.VMEM((n, ncol), bf16),
            pltpu.VMEM((side, 8, LANES), f32),
            pltpu.VMEM((side, 8, LANES), f32),
            pltpu.VMEM((2, 8, LANES), f32),
            dma((chunks + 3,)),
            dma((far,)),
            dma((2,)),
            dma((chunks, 2, 2, far)),
            dma((chunks, 2, 2, far)),
            dma((chunks, 2, 2, far, side)),
            dma((chunks, 2, 2, far, side)),
            dma((chunks, 2, 2, far, units)),
            dma((chunks, 2, 2, far, units)),
            dma((chunks, 2, side, units)),
            dma((chunks, 2, side, units)),
            dma((rest, far)),
            dma((band,)),
            dma((far, side)),
            dma((far, 2)),
            dma((side - 1,)),
            dma((side - 1,)),
            dma((side - 1,)),
            dma((side - 1,)),
            dma,
            dma,
        ],
        compiler_params=pltpu.CompilerParams(
            collective_id=0, has_side_effects=True, vmem_limit_bytes=60 * 1024 * 1024
        ),
        name="fock",
    )(factors, orbitals, field_term)


def solution(mesh):
    side = math.isqrt(mesh.shape["row"])
    finer = Mesh(
        mesh.devices.reshape(mesh.shape["grp"], side, side, mesh.shape["col"]),
        ("grp", "row_0", "row_1", "col"),
    )
    return jax.shard_map(
        functools.partial(shards, side, CHUNKS),
        mesh=finer,
        in_specs=(P(None, GRP_ROW, "col"), P(GRP_ROW, "col"), P(GRP_ROW, "col")),
        out_specs=P(GRP_ROW, "col"),
        check_vma=False,
    )
```
